32 devices in a mesh: date: 16 (over z, y, x), pix: 2 (over core).
Axes of the slice: x: 2, y: 2, z: 4, core: 2. Of those that a mesh axis runs over, the one named last changes fastest.
Arguments:
- reflect: bfloat16 [64, 6, 16384], P('date', None, 'pix'), may hold values from -8 to 8
- cloud_free: int32 [64, 16384], P('date', 'pix'), may hold values from 0 to 1, as said below
- days: int32 [64], P('date'), may hold values from 1 to 2079, as said below
Outputs:
- median: float32 [6, 16384], P(None, 'pix')
- slope: float32 [6, 16384], P(None, 'pix')
The draws below stay inside these ranges and needn't reach their ends.
Inputs may be any that keep to these rules, and one draw needn't show every extreme that they name: `cloud_free`: every pixel is clear on at least one of the first 32 dates and on at least one of the others; clear shares differ between tiles. `days`: strictly increasing.
All inputs are finite; a program needn't handle non-finite values.
Results may differ from the reference program's by a relative error of at most 0.0003.
Values may be sent and summed in bfloat16 or wider, within the bound.
A program may use at most 64 MiB of HBM per device.

```python
import jax
import jax.numpy as jnp
from jax import lax

DATES = 64
BANDS = 6
PIX_DEV = 8192
PIXELS = 16384


def draw_reflect(key, part):
    keys = jax.random.split(key, 4)
    tiles = PIXELS // PIX_DEV
    region = jax.random.normal(keys[0], (1, BANDS, tiles), jnp.float32)
    haze = 0.6 * jax.random.normal(keys[1], (DATES, BANDS, 1), jnp.float32)
    tile_date = 0.5 * jax.random.normal(keys[2], (DATES, BANDS, tiles), jnp.float32)
    base = jnp.repeat(region + tile_date, PIX_DEV, axis=2) + haze
    noise = 0.8 * jax.random.normal(keys[3], (DATES, BANDS, PIXELS), jnp.float32)
    return jnp.clip(base + noise, -8.0, 8.0).astype(jnp.bfloat16)


def draw_cloud_free(key, part):
    keys = jax.random.split(key, 4)
    tiles = PIXELS // PIX_DEV
    cloudy = jnp.repeat(jax.random.randint(keys[0], (tiles,), 10, 85), PIX_DEV)
    rolls = jax.random.randint(keys[1], (DATES, PIXELS), 0, 100)
    clear = rolls >= cloudy[None, :]
    first = jax.random.randint(keys[2], (PIXELS,), 0, DATES // 2)
    second = jax.random.randint(keys[3], (PIXELS,), DATES // 2, DATES)
    rows = jnp.arange(DATES, dtype=jnp.int32)[:, None]
    clear = clear | (rows == first[None, :]) | (rows == second[None, :])
    return clear.astype(jnp.int32)


def draw_days(key, part):
    keys = jax.random.split(key, 2)
    start = jax.random.randint(keys[0], (), 0, 31)
    gaps = jax.random.randint(keys[1], (DATES,), 1, 33)
    raw = (start + jnp.cumsum(gaps)).astype(jnp.int32)
    index = jnp.arange(DATES, dtype=jnp.int32)
    raw = jnp.where(index == 0, jnp.int32(1), raw)
    raw = jnp.where(index == DATES - 1, jnp.int32(31 + 32 * DATES), raw)
    return raw.astype(jnp.int32)


def setup_inputs(seed: int = 0) -> dict:
    arg_keys = jax.random.split(jax.random.key(seed), 4)
    reflect = draw_reflect(jax.random.fold_in(arg_keys[3], 71), 0)
    cloud_free = draw_cloud_free(jax.random.fold_in(arg_keys[3], 71), 0)
    days = draw_days(jax.random.fold_in(arg_keys[3], 71), 0)
    return {"reflect": reflect, "cloud_free": cloud_free, "days": days}


ridge = 1.0


def rank_block(pair):
    xb, mb = pair
    zeros = jnp.zeros(xb.shape, jnp.float32)

    def step(i, carry):
        less, equal = carry
        xt = lax.dynamic_index_in_dim(xb, i, 0, keepdims=True)
        mt = lax.dynamic_index_in_dim(mb, i, 0, keepdims=True)[:, None, :]
        less = less + mt * (xt < xb).astype(jnp.float32)
        equal = equal + mt * (xt == xb).astype(jnp.float32)
        return (less, equal)

    less, equal = lax.fori_loop(0, xb.shape[0], step, (zeros, zeros))
    count = jnp.sum(mb, 0)
    lower = jnp.floor((count - 1.0) / 2.0)
    upper = jnp.floor(count / 2.0)

    def pick(level):
        chosen = mb[:, None, :] * ((less <= level) & (level < less + equal)).astype(jnp.float32)
        return jnp.sum(chosen * xb, 0) / jnp.maximum(jnp.sum(chosen, 0), 1.0)

    return 0.5 * (pick(lower) + pick(upper))


def reference(reflect, cloud_free, days):
    x = reflect.astype(jnp.float32)
    m = cloud_free.astype(jnp.float32)
    t = days.astype(jnp.float32) / 365.0
    csum = jnp.sum(x * m[:, None, :], 2)
    cnt = jnp.sum(m, 1)
    scene_mean = csum / jnp.maximum(cnt, 1.0)[:, None]
    y = x - scene_mean[:, :, None]
    s0 = jnp.sum(m, 0)
    s1 = jnp.sum(t[:, None] * m, 0)
    s2 = jnp.sum((t * t)[:, None] * m, 0)
    sy = jnp.sum(m[:, None, :] * y, 0)
    sty = jnp.sum((t[:, None] * m)[:, None, :] * y, 0)
    first = s0 + ridge
    det = first * (s2 + ridge) - s1 * s1
    slope = (first[None, :] * sty - s1[None, :] * sy) / det[None, :]
    blocks = PIXELS // PIX_DEV
    xs = x.reshape(DATES, BANDS, blocks, PIX_DEV).transpose(2, 0, 1, 3)
    ms = m.reshape(DATES, blocks, PIX_DEV).transpose(1, 0, 2)
    med = lax.map(rank_block, (xs, ms))
    median = med.transpose(1, 0, 2).reshape(BANDS, PIXELS)
    return median, slope
```

```python
import functools

import jax
import jax.numpy as jnp
from jax import lax
from jax.experimental import pallas as pl
from jax.experimental.pallas import tpu as pltpu
from jax.sharding import PartitionSpec as P

MESH = pl.DeviceIdType.MESH
ridge = 1.0
sentinel = 100.0
lanes = 128
slot = 8


def merge_pairs(lo, hi, r):
    step = r * 2
    if step < hi - lo:
        yield from merge_pairs(lo, hi, step)
        yield from merge_pairs(lo + r, hi, step)
        yield from ((i, i + r) for i in range(lo + r, hi - r, step))
    else:
        yield (lo, lo + r)


def sort_pairs(lo, hi):
    if hi - lo >= 1:
        mid = lo + (hi - lo) // 2
        yield from sort_pairs(lo, mid)
        yield from sort_pairs(mid + 1, hi)
        yield from merge_pairs(lo, hi, 1)


def sort_network(values):
    values = list(values)
    for i, j in sort_pairs(0, len(values) - 1):
        a, b = values[i], values[j]
        values[i], values[j] = jnp.minimum(a, b), jnp.maximum(a, b)
    return values


def kernel(
    n,
    pixes,
    spans,
    x_hbm,
    m_hbm,
    days_ref,
    out_ref,
    x_ref,
    m_ref,
    wide,
    sent,
    got,
    part,
    parts,
    mean_row,
    mean_rows,
    stack,
    mean_tile,
    year_tile,
    flip,
    odd,
    slopes,
    coded,
    load_sem,
    data_send,
    data_recv,
    part_send,
    part_recv,
    mean_send,
    mean_recv,
    code_send,
    code_recv,
    *code,
):
    me = lax.axis_index("date")
    pix = lax.axis_index("pix")
    bands, dates, tile = x_ref.shape
    width = tile // n
    total = n * dates
    starts = [sum(spans[:p]) for p in range(len(spans))]

    def ahead(r):
        return lax.rem(me + r, n)

    def behind(r):
        return lax.rem(me + n - r, n)

    barrier = pltpu.get_barrier_semaphore()

    @pl.loop(1, n)
    def _(r):
        pl.semaphore_signal(barrier, inc=1, device_id={"date": ahead(r)}, device_id_type=MESH)

    for r in range(1, pixes):
        pl.semaphore_signal(barrier, inc=1, device_id={"pix": lax.rem(pix + r, pixes)}, device_id_type=MESH)

    load_x = pltpu.make_async_copy(x_hbm, x_ref, load_sem.at[0])
    load_m = pltpu.make_async_copy(m_hbm, m_ref, load_sem.at[1])
    load_x.start()
    load_m.start()
    stack[...] = jnp.zeros_like(stack)
    coded[...] = jnp.zeros_like(coded)
    load_m.wait()
    load_x.wait()

    def mark(j, carry):
        cols = pl.ds(pl.multiple_of(j * width, lanes), width)
        valid = m_ref[:, cols] > 0
        out = []
        for b in range(bands):
            x = x_ref[b, :, cols].astype(jnp.float32)
            marked = jnp.where(valid, x, sentinel)
            for d in range(dates):
                wide[d * bands + b : d * bands + b + 1, :] = marked[d : d + 1, :]
            out.append(carry[b] + jnp.where(valid, x, 0.0))
        sent[j] = wide[...].astype(jnp.bfloat16)
        out.append(carry[bands] + jnp.where(valid, 1.0, 0.0))
        return tuple(out)

    zero = jnp.zeros((dates, width), jnp.float32)
    sums = lax.fori_loop(0, n, mark, tuple(zero for _ in range(bands + 1)))
    got[me] = sent[me]

    lane = lax.broadcasted_iota(jnp.int32, (dates, lanes), 1)
    date = lax.broadcasted_iota(jnp.int32, (dates, lanes), 0)
    lane_row = lax.broadcasted_iota(jnp.int32, (1, lanes), 1)
    row = jnp.zeros((dates, lanes), jnp.float32)
    for b in range(bands):
        row = row + jnp.where(lane == date * slot + b, jnp.sum(sums[b], axis=1, keepdims=True), 0.0)
    own = (lane >= date * slot) & (lane < (date + 1) * slot)
    count_row = jnp.where(own, jnp.sum(sums[bands], axis=1, keepdims=True), 0.0)
    part[0:1, :] = jnp.sum(row, axis=0, keepdims=True)
    part[1:2, :] = jnp.sum(count_row, axis=0, keepdims=True)
    years = jnp.zeros((1, lanes), jnp.float32)
    for d in range(dates):
        year = jnp.full((1, lanes), days_ref[d], jnp.int32).astype(jnp.float32) / 365.0
        years = jnp.where((lane_row >= d * slot) & (lane_row < (d + 1) * slot), year, years)
    mean_row[1:2, :] = years

    def part_copy(r):
        return pltpu.make_async_remote_copy(
            src_ref=part,
            dst_ref=parts.at[r],
            send_sem=part_send.at[r],
            recv_sem=part_recv.at[r],
            device_id={"pix": lax.rem(pix + r, pixes)},
            device_id_type=MESH,
        )

    def data_copy(r):
        return pltpu.make_async_remote_copy(
            src_ref=sent.at[ahead(r)],
            dst_ref=got.at[me],
            send_sem=data_send.at[r],
            recv_sem=data_recv.at[r],
            device_id={"date": ahead(r)},
            device_id_type=MESH,
        )

    def mean_copy(r):
        return pltpu.make_async_remote_copy(
            src_ref=mean_row,
            dst_ref=mean_rows.at[me],
            send_sem=mean_send.at[r],
            recv_sem=mean_recv.at[r],
            device_id={"date": ahead(r)},
            device_id_type=MESH,
        )

    def code_copy(p, r):
        return pltpu.make_async_remote_copy(
            src_ref=code[p].at[me],
            dst_ref=code[p].at[me],
            send_sem=code_send.at[p, r],
            recv_sem=code_recv.at[p, r],
            device_id={"date": ahead(r)},
            device_id_type=MESH,
        )

    early = min(4, n)
    pl.semaphore_wait(barrier, n - 1 + pixes - 1)
    for r in range(1, pixes):
        part_copy(r).start()

    @pl.loop(1, early)
    def _(r):
        data_copy(r).start()

    csum_row = part[0:1, :]
    cnt_row = part[1:2, :]
    for r in range(1, pixes):
        part_copy(r).wait_recv()
        csum_row = csum_row + parts[r, 0:1, :]
        cnt_row = cnt_row + parts[r, 1:2, :]
    mean_row[0:1, :] = csum_row / jnp.maximum(cnt_row, 1.0)
    mean_rows[me] = mean_row[...]

    @pl.loop(1, n)
    def _(r):
        mean_copy(r).start()

    @pl.loop(early, n)
    def _(r):
        data_copy(r).start()

    @pl.loop(1, n)
    def _(r):
        mean_copy(r).wait_recv()

    for row_index, tile_ref in ((0, mean_tile), (1, year_tile)):
        for j in range(n):
            stack[j : j + 1, :] = mean_rows[j, row_index : row_index + 1, :]
        turned = jnp.transpose(stack[...])
        for j in range(n):
            for d in range(dates):
                column = turned[d * slot : d * slot + bands, j : j + 1]
                tile_ref[j * dates + d] = jnp.broadcast_to(column, (bands, lanes))

    def trend(r, carry):
        j = behind(r)
        fill, s_zero, s_one, s_two, s_y, s_ty = carry
        block = got[j].astype(jnp.float32)
        for d in range(dates):
            x = block[d * bands : (d + 1) * bands, :]
            year = jnp.concatenate([year_tile[j * dates + d]] * (width // lanes), axis=1)
            mean = jnp.concatenate([mean_tile[j * dates + d]] * (width // lanes), axis=1)
            valid = x < 50.0
            y = jnp.where(valid, x - mean, 0.0)
            m = jnp.where(valid, 1.0, 0.0)
            tm = year * m
            s_zero = s_zero + m
            s_one = s_one + tm
            s_two = s_two + year * tm
            s_y = s_y + y
            s_ty = s_ty + year * y
            flip[r * dates + d] = jnp.where(valid, x, fill)
            fill = jnp.where(valid, fill, -fill)
        return (fill, s_zero, s_one, s_two, s_y, s_ty)

    def arrived(r, carry):
        data_copy(r).wait_recv()
        return trend(r, carry)

    half = total // 2
    blank = jnp.zeros((bands, width), jnp.float32)
    sums = trend(0, (blank + sentinel, blank, blank, blank, blank, blank))
    sums = lax.fori_loop(1, n // 2, arrived, sums)

    @pl.loop(0, width // lanes)
    def _(k):
        cols = pl.ds(pl.multiple_of(k * lanes, lanes), lanes)
        for i, value in enumerate(sort_network([flip[i, :, cols] for i in range(half)])):
            flip[i, :, cols] = value

    sums = lax.fori_loop(n // 2, n, arrived, sums)
    fill, s_zero, s_one, s_two, s_y, s_ty = sums
    first = s_zero + ridge
    slopes[...] = (first * s_ty - s_one * s_y) / (first * (s_two + ridge) - s_one * s_one)
    odd[...] = jnp.where(fill < 0.0, 1.0, 0.0)

    def encode(base, values):
        top = jnp.maximum(jnp.max(jnp.abs(values), axis=0, keepdims=True), 1e-30)
        power = jnp.floor(jnp.log2(top))
        whole = jnp.round(values * jnp.exp2(14.0 - power))
        coded[base : base + bands, :] = jnp.clip(whole, -32767.0, 32767.0)
        coded[base + bands : base + bands + 1, :] = power

    def decode(p, j):
        for k in range(spans[p] // lanes):
            values = code[p][j, :, k * lanes : (k + 1) * lanes].astype(jnp.int32).astype(jnp.float32)
            there = pl.ds(pl.multiple_of(j * width + starts[p] + k * lanes, lanes), lanes)
            for o in range(2):
                scale = jnp.exp2(values[o * slot + bands : o * slot + bands + 1, :] - 14.0)
                out_ref[o, :, there] = values[o * slot : o * slot + bands, :] * scale

    for p, span in enumerate(spans):

        @pl.loop(0, span // lanes)
        def _(k):
            cols = pl.ds(pl.multiple_of(starts[p] + k * lanes, lanes), lanes)
            here = pl.ds(pl.multiple_of(k * lanes, lanes), lanes)
            low = [flip[i, :, cols] for i in range(half)]
            high = sort_network([flip[half + i, :, cols] for i in range(half)])
            lower = None
            upper = None
            for i in range(half):
                a, b = low[i], high[half - 1 - i]
                small, large = jnp.minimum(a, b), jnp.maximum(a, b)
                lower = small if lower is None else jnp.maximum(lower, small)
                upper = large if upper is None else jnp.minimum(upper, large)
            median = jnp.where(odd[:, cols] > 0.5, lower, 0.5 * (lower + upper))
            encode(0, median)
            encode(slot, slopes[:, cols])
            code[p][me, :, here] = coded[...].astype(jnp.int32).astype(jnp.int16)

        @pl.loop(1, n)
        def _(r):
            code_copy(p, r).start()

    for p in range(len(spans)):
        decode(p, me)

        @pl.loop(1, n)
        def _(r):
            code_copy(p, r).wait_recv()
            decode(p, behind(r))

    for r in range(1, pixes):
        part_copy(r).wait_send()

    @pl.loop(1, n)
    def _(r):
        mean_copy(r).wait_send()
        data_copy(r).wait_send()
        for p in range(len(spans)):
            code_copy(p, r).wait_send()


def local(n, pixes, reflect, cloud_free, days):
    dates, bands, tile = reflect.shape
    width = tile // n
    spans = [width]
    turned = -(-n // lanes) * lanes
    vmem = pl.BlockSpec(memory_space=pltpu.VMEM)
    hbm = pl.BlockSpec(memory_space=pl.ANY)
    dma = pltpu.SemaphoreType.DMA
    out = pl.pallas_call(
        functools.partial(kernel, n, pixes, spans),
        out_shape=pltpu.VMEM((2, bands, tile), jnp.float32),
        in_specs=[hbm, hbm, pl.BlockSpec(memory_space=pltpu.SMEM)],
        out_specs=vmem,
        scratch_shapes=[
            pltpu.VMEM((bands, dates, tile), jnp.bfloat16),
            pltpu.VMEM((dates, tile), jnp.int32),
            pltpu.VMEM((dates * bands, width), jnp.float32),
            pltpu.VMEM((n, dates * bands, width), jnp.bfloat16),
            pltpu.VMEM((n, dates * bands, width), jnp.bfloat16),
            pltpu.VMEM((2, lanes), jnp.float32),
            pltpu.VMEM((pixes, 2, lanes), jnp.float32),
            pltpu.VMEM((2, lanes), jnp.float32),
            pltpu.VMEM((n, 2, lanes), jnp.float32),
            pltpu.VMEM((turned, lanes), jnp.float32),
            pltpu.VMEM((n * dates, bands, lanes), jnp.float32),
            pltpu.VMEM((n * dates, bands, lanes), jnp.float32),
            pltpu.VMEM((n * dates, bands, width), jnp.float32),
            pltpu.VMEM((bands, width), jnp.float32),
            pltpu.VMEM((bands, width), jnp.float32),
            pltpu.VMEM((2 * slot, lanes), jnp.float32),
            dma((2,)),
            dma((n,)),
            dma((n,)),
            dma((pixes,)),
            dma((pixes,)),
            dma((n,)),
            dma((n,)),
            dma((len(spans), n)),
            dma((len(spans), n)),
            *[pltpu.VMEM((n, 2 * slot, span), jnp.int16) for span in spans],
        ],
        compiler_params=pltpu.CompilerParams(collective_id=0, has_side_effects=True),
    )(jnp.transpose(reflect, (1, 0, 2)), cloud_free, days)
    return (out[0], out[1])


def solution(mesh):
    placed = (P("date", None, "pix"), P("date", "pix"), P("date"))
    return jax.shard_map(
        functools.partial(local, mesh.shape["date"], mesh.shape["pix"]),
        mesh=mesh,
        in_specs=placed,
        out_specs=(P(None, "pix"), P(None, "pix")),
        check_vma=False,
    )
```

```python
import functools

import jax
import jax.numpy as jnp
from jax import lax
from jax.experimental import pallas as pl
from jax.experimental.pallas import tpu as pltpu
from jax.sharding import PartitionSpec as P

MESH = pl.DeviceIdType.MESH
ridge = 1.0
sentinel = 100.0
lanes = 128
slot = 8


def merge_pairs(lo, hi, r):
    step = r * 2
    if step < hi - lo:
        yield from merge_pairs(lo, hi, step)
        yield from merge_pairs(lo + r, hi, step)
        yield from ((i, i + r) for i in range(lo + r, hi - r, step))
    else:
        yield (lo, lo + r)


def sort_pairs(lo, hi):
    if hi - lo >= 1:
        mid = lo + (hi - lo) // 2
        yield from sort_pairs(lo, mid)
        yield from sort_pairs(mid + 1, hi)
        yield from merge_pairs(lo, hi, 1)


def sort_network(values):
    values = list(values)
    for i, j in sort_pairs(0, len(values) - 1):
        a, b = values[i], values[j]
        values[i], values[j] = jnp.minimum(a, b), jnp.maximum(a, b)
    return values


def kernel(
    n,
    pixes,
    group,
    spans,
    x_hbm,
    m_hbm,
    days_ref,
    out_ref,
    x_ref,
    m_ref,
    wide,
    sent,
    got,
    part,
    parts,
    mean_row,
    mean_rows,
    stack,
    mean_tile,
    year_tile,
    flip,
    odd,
    slopes,
    coded,
    plane_sem,
    load_sem,
    data_send,
    data_recv,
    part_send,
    part_recv,
    mean_send,
    mean_recv,
    code_send,
    code_recv,
    *code,
):
    me = lax.axis_index("date")
    pix = lax.axis_index("pix")
    bands, dates, tile = x_ref.shape
    width = tile // n
    total = n * dates
    starts = [sum(spans[:p]) for p in range(len(spans))]

    lines = n // group
    line = me // group
    spot = lax.rem(me, group)

    def ahead(r):
        return lax.rem(line + r // group, lines) * group + lax.rem(spot + lax.rem(r, group), group)

    def behind(r):
        return lax.rem(line + lines - r // group, lines) * group + lax.rem(spot + group - lax.rem(r, group), group)

    stack_line = [a * group for a in range(1, lines)]
    plane = list(range(1, group))
    rest = [r for r in range(1, n) if r not in stack_line and r not in plane]

    barrier = pltpu.get_barrier_semaphore()
    for r in stack_line + plane:
        pl.semaphore_signal(barrier, inc=1, device_id={"date": ahead(r)}, device_id_type=MESH)
    for r in range(1, pixes):
        pl.semaphore_signal(barrier, inc=1, device_id={"pix": lax.rem(pix + r, pixes)}, device_id_type=MESH)

    load_x = pltpu.make_async_copy(x_hbm, x_ref, load_sem.at[0])
    load_m = pltpu.make_async_copy(m_hbm, m_ref, load_sem.at[1])
    load_x.start()
    load_m.start()
    stack[...] = jnp.zeros_like(stack)
    coded[...] = jnp.zeros_like(coded)
    load_m.wait()
    load_x.wait()

    def mark(j, carry):
        cols = pl.ds(pl.multiple_of(j * width, lanes), width)
        valid = m_ref[:, cols] > 0
        out = []
        for b in range(bands):
            x = x_ref[b, :, cols].astype(jnp.float32)
            marked = jnp.where(valid, x, sentinel)
            for d in range(dates):
                wide[d * bands + b : d * bands + b + 1, :] = marked[d : d + 1, :]
            out.append(carry[b] + jnp.where(valid, x, 0.0))
        sent[j] = wide[...].astype(jnp.bfloat16)
        out.append(carry[bands] + jnp.where(valid, 1.0, 0.0))
        return tuple(out)

    zero = jnp.zeros((dates, width), jnp.float32)
    sums = lax.fori_loop(0, n, mark, tuple(zero for _ in range(bands + 1)))
    got[me] = sent[me]

    lane = lax.broadcasted_iota(jnp.int32, (dates, lanes), 1)
    date = lax.broadcasted_iota(jnp.int32, (dates, lanes), 0)
    lane_row = lax.broadcasted_iota(jnp.int32, (1, lanes), 1)
    row = jnp.zeros((dates, lanes), jnp.float32)
    for b in range(bands):
        row = row + jnp.where(lane == date * slot + b, jnp.sum(sums[b], axis=1, keepdims=True), 0.0)
    own = (lane >= date * slot) & (lane < (date + 1) * slot)
    count_row = jnp.where(own, jnp.sum(sums[bands], axis=1, keepdims=True), 0.0)
    part[0:1, :] = jnp.sum(row, axis=0, keepdims=True)
    part[1:2, :] = jnp.sum(count_row, axis=0, keepdims=True)
    years = jnp.zeros((1, lanes), jnp.float32)
    for d in range(dates):
        year = jnp.full((1, lanes), days_ref[d], jnp.int32).astype(jnp.float32) / 365.0
        years = jnp.where((lane_row >= d * slot) & (lane_row < (d + 1) * slot), year, years)
    mean_row[1:2, :] = years

    def part_copy(r):
        return pltpu.make_async_remote_copy(
            src_ref=part,
            dst_ref=parts.at[r],
            send_sem=part_send.at[r],
            recv_sem=part_recv.at[r],
            device_id={"pix": lax.rem(pix + r, pixes)},
            device_id_type=MESH,
        )

    def data_copy(r):
        return pltpu.make_async_remote_copy(
            src_ref=sent.at[ahead(r)],
            dst_ref=got.at[me],
            send_sem=data_send.at[r],
            recv_sem=data_recv.at[r],
            device_id={"date": ahead(r)},
            device_id_type=MESH,
        )

    def mean_copy(r):
        return pltpu.make_async_remote_copy(
            src_ref=mean_row,
            dst_ref=mean_rows.at[me],
            send_sem=mean_send.at[r],
            recv_sem=mean_recv.at[r],
            device_id={"date": ahead(r)},
            device_id_type=MESH,
        )

    def code_copy(p, r):
        return pltpu.make_async_remote_copy(
            src_ref=code[p].at[me],
            dst_ref=code[p].at[me],
            send_sem=code_send.at[p, r],
            recv_sem=code_recv.at[p, r],
            device_id={"date": ahead(r)},
            device_id_type=MESH,
        )

    pl.semaphore_wait(barrier, len(stack_line) + len(plane) + pixes - 1)
    for r in plane:
        pl.semaphore_signal(plane_sem, inc=1, device_id={"date": ahead(r)}, device_id_type=MESH)
    for r in range(1, pixes):
        part_copy(r).start()
    for r in stack_line + plane:
        data_copy(r).start()

    csum_row = part[0:1, :]
    cnt_row = part[1:2, :]
    for r in range(1, pixes):
        part_copy(r).wait_recv()
        csum_row = csum_row + parts[r, 0:1, :]
        cnt_row = cnt_row + parts[r, 1:2, :]
    mean_row[0:1, :] = csum_row / jnp.maximum(cnt_row, 1.0)
    mean_rows[me] = mean_row[...]
    pl.semaphore_wait(plane_sem, len(plane))
    for r in range(1, n):
        mean_copy(r).start()
    for r in rest:
        data_copy(r).start()

    @pl.loop(1, n)
    def _(r):
        mean_copy(r).wait_recv()

    for row_index, tile_ref in ((0, mean_tile), (1, year_tile)):
        for j in range(n):
            stack[j : j + 1, :] = mean_rows[j, row_index : row_index + 1, :]
        turned = jnp.transpose(stack[...])
        for j in range(n):
            for d in range(dates):
                column = turned[d * slot : d * slot + bands, j : j + 1]
                tile_ref[j * dates + d] = jnp.broadcast_to(column, (bands, lanes))

    def trend(r, carry):
        j = behind(r)
        fill, s_zero, s_one, s_two, s_y, s_ty = carry
        block = got[j].astype(jnp.float32)
        for d in range(dates):
            x = block[d * bands : (d + 1) * bands, :]
            year = jnp.concatenate([year_tile[j * dates + d]] * (width // lanes), axis=1)
            mean = jnp.concatenate([mean_tile[j * dates + d]] * (width // lanes), axis=1)
            valid = x < 50.0
            y = jnp.where(valid, x - mean, 0.0)
            m = jnp.where(valid, 1.0, 0.0)
            tm = year * m
            s_zero = s_zero + m
            s_one = s_one + tm
            s_two = s_two + year * tm
            s_y = s_y + y
            s_ty = s_ty + year * y
            flip[r * dates + d] = jnp.where(valid, x, fill)
            fill = jnp.where(valid, fill, -fill)
        return (fill, s_zero, s_one, s_two, s_y, s_ty)

    def arrived(r, carry):
        data_copy(r).wait_recv()
        return trend(r, carry)

    half = total // 2
    blank = jnp.zeros((bands, width), jnp.float32)
    sums = trend(0, (blank + sentinel, blank, blank, blank, blank, blank))
    sums = lax.fori_loop(1, n // 2, arrived, sums)

    @pl.loop(0, width // lanes)
    def _(k):
        cols = pl.ds(pl.multiple_of(k * lanes, lanes), lanes)
        for i, value in enumerate(sort_network([flip[i, :, cols] for i in range(half)])):
            flip[i, :, cols] = value

    sums = lax.fori_loop(n // 2, n, arrived, sums)
    fill, s_zero, s_one, s_two, s_y, s_ty = sums
    first = s_zero + ridge
    slopes[...] = (first * s_ty - s_one * s_y) / (first * (s_two + ridge) - s_one * s_one)
    odd[...] = jnp.where(fill < 0.0, 1.0, 0.0)

    def encode(base, values):
        top = jnp.maximum(jnp.max(jnp.abs(values), axis=0, keepdims=True), 1e-30)
        power = jnp.floor(jnp.log2(top))
        whole = jnp.round(values * jnp.exp2(14.0 - power))
        coded[base : base + bands, :] = jnp.clip(whole, -32767.0, 32767.0)
        coded[base + bands : base + bands + 1, :] = power

    def decode(p, j):
        for k in range(spans[p] // lanes):
            values = code[p][j, :, k * lanes : (k + 1) * lanes].astype(jnp.int32).astype(jnp.float32)
            there = pl.ds(pl.multiple_of(j * width + starts[p] + k * lanes, lanes), lanes)
            for o in range(2):
                scale = jnp.exp2(values[o * slot + bands : o * slot + bands + 1, :] - 14.0)
                out_ref[o, :, there] = values[o * slot : o * slot + bands, :] * scale

    for p, span in enumerate(spans):

        @pl.loop(0, span // lanes)
        def _(k):
            cols = pl.ds(pl.multiple_of(starts[p] + k * lanes, lanes), lanes)
            here = pl.ds(pl.multiple_of(k * lanes, lanes), lanes)
            low = [flip[i, :, cols] for i in range(half)]
            high = sort_network([flip[half + i, :, cols] for i in range(half)])
            lower = None
            upper = None
            for i in range(half):
                a, b = low[i], high[half - 1 - i]
                small, large = jnp.minimum(a, b), jnp.maximum(a, b)
                lower = small if lower is None else jnp.maximum(lower, small)
                upper = large if upper is None else jnp.minimum(upper, large)
            median = jnp.where(odd[:, cols] > 0.5, lower, 0.5 * (lower + upper))
            encode(0, median)
            encode(slot, slopes[:, cols])
            code[p][me, :, here] = coded[...].astype(jnp.int32).astype(jnp.int16)

        @pl.loop(1, n)
        def _(r):
            code_copy(p, r).start()

    for p in range(len(spans)):
        decode(p, me)

        @pl.loop(1, n)
        def _(r):
            code_copy(p, r).wait_recv()
            decode(p, behind(r))

    for r in range(1, pixes):
        part_copy(r).wait_send()

    @pl.loop(1, n)
    def _(r):
        mean_copy(r).wait_send()
        data_copy(r).wait_send()
        for p in range(len(spans)):
            code_copy(p, r).wait_send()


def local(n, pixes, reflect, cloud_free, days):
    dates, bands, tile = reflect.shape
    width = tile // n
    spans = [width]
    group = 1
    while group * group * 4 <= n and n % (group * 2) == 0:
        group *= 2
    turned = -(-n // lanes) * lanes
    vmem = pl.BlockSpec(memory_space=pltpu.VMEM)
    hbm = pl.BlockSpec(memory_space=pl.ANY)
    dma = pltpu.SemaphoreType.DMA
    out = pl.pallas_call(
        functools.partial(kernel, n, pixes, group, spans),
        out_shape=pltpu.VMEM((2, bands, tile), jnp.float32),
        in_specs=[hbm, hbm, pl.BlockSpec(memory_space=pltpu.SMEM)],
        out_specs=vmem,
        scratch_shapes=[
            pltpu.VMEM((bands, dates, tile), jnp.bfloat16),
            pltpu.VMEM((dates, tile), jnp.int32),
            pltpu.VMEM((dates * bands, width), jnp.float32),
            pltpu.VMEM((n, dates * bands, width), jnp.bfloat16),
            pltpu.VMEM((n, dates * bands, width), jnp.bfloat16),
            pltpu.VMEM((2, lanes), jnp.float32),
            pltpu.VMEM((pixes, 2, lanes), jnp.float32),
            pltpu.VMEM((2, lanes), jnp.float32),
            pltpu.VMEM((n, 2, lanes), jnp.float32),
            pltpu.VMEM((turned, lanes), jnp.float32),
            pltpu.VMEM((n * dates, bands, lanes), jnp.float32),
            pltpu.VMEM((n * dates, bands, lanes), jnp.float32),
            pltpu.VMEM((n * dates, bands, width), jnp.float32),
            pltpu.VMEM((bands, width), jnp.float32),
            pltpu.VMEM((bands, width), jnp.float32),
            pltpu.VMEM((2 * slot, lanes), jnp.float32),
            pltpu.SemaphoreType.REGULAR,
            dma((2,)),
            dma((n,)),
            dma((n,)),
            dma((pixes,)),
            dma((pixes,)),
            dma((n,)),
            dma((n,)),
            dma((len(spans), n)),
            dma((len(spans), n)),
            *[pltpu.VMEM((n, 2 * slot, span), jnp.int16) for span in spans],
        ],
        compiler_params=pltpu.CompilerParams(collective_id=0, has_side_effects=True),
    )(jnp.transpose(reflect, (1, 0, 2)), cloud_free, days)
    return (out[0], out[1])


def solution(mesh):
    placed = (P("date", None, "pix"), P("date", "pix"), P("date"))
    return jax.shard_map(
        functools.partial(local, mesh.shape["date"], mesh.shape["pix"]),
        mesh=mesh,
        in_specs=placed,
        out_specs=(P(None, "pix"), P(None, "pix")),
        check_vma=False,
    )
```

```python
import functools

import jax
import jax.numpy as jnp
from jax import lax
from jax.experimental import pallas as pl
from jax.experimental.pallas import tpu as pltpu
from jax.sharding import PartitionSpec as P

MESH = pl.DeviceIdType.MESH
ridge = 1.0
sentinel = 100.0
lanes = 128
slot = 8


def merge_pairs(lo, hi, r):
    step = r * 2
    if step < hi - lo:
        yield from merge_pairs(lo, hi, step)
        yield from merge_pairs(lo + r, hi, step)
        yield from ((i, i + r) for i in range(lo + r, hi - r, step))
    else:
        yield (lo, lo + r)


def sort_pairs(lo, hi):
    if hi - lo >= 1:
        mid = lo + (hi - lo) // 2
        yield from sort_pairs(lo, mid)
        yield from sort_pairs(mid + 1, hi)
        yield from merge_pairs(lo, hi, 1)


def sort_network(values):
    values = list(values)
    for i, j in sort_pairs(0, len(values) - 1):
        a, b = values[i], values[j]
        values[i], values[j] = jnp.minimum(a, b), jnp.maximum(a, b)
    return values


def kernel(
    n,
    pixes,
    group,
    spans,
    x_hbm,
    m_hbm,
    days_ref,
    out_ref,
    x_ref,
    m_ref,
    wide,
    sent,
    got,
    part,
    parts,
    mean_row,
    mean_rows,
    stack,
    mean_tile,
    year_tile,
    flip,
    odd,
    slopes,
    coded,
    plane_sem,
    load_sem,
    data_send,
    data_recv,
    part_send,
    part_recv,
    mean_send,
    mean_recv,
    code_send,
    code_recv,
    *code,
):
    me = lax.axis_index("date")
    pix = lax.axis_index("pix")
    bands, dates, tile = x_ref.shape
    width = tile // n
    total = n * dates
    starts = [sum(spans[:p]) for p in range(len(spans))]

    lines = n // group
    line = me // group
    spot = lax.rem(me, group)

    def ahead(r):
        return lax.rem(line + r // group, lines) * group + lax.rem(spot + lax.rem(r, group), group)

    def behind(r):
        return lax.rem(line + lines - r // group, lines) * group + lax.rem(spot + group - lax.rem(r, group), group)

    stack_line = [a * group for a in range(1, lines)]
    plane = list(range(1, group))
    rest = [r for r in range(1, n) if r not in stack_line and r not in plane]

    barrier = pltpu.get_barrier_semaphore()
    for r in stack_line + plane:
        pl.semaphore_signal(barrier, inc=1, device_id={"date": ahead(r)}, device_id_type=MESH)
    for r in range(1, pixes):
        pl.semaphore_signal(barrier, inc=1, device_id={"pix": lax.rem(pix + r, pixes)}, device_id_type=MESH)

    load_x = pltpu.make_async_copy(x_hbm, x_ref, load_sem.at[0])
    load_m = pltpu.make_async_copy(m_hbm, m_ref, load_sem.at[1])
    load_x.start()
    load_m.start()
    stack[...] = jnp.zeros_like(stack)
    coded[...] = jnp.zeros_like(coded)
    load_m.wait()
    load_x.wait()

    def mark(j, carry):
        cols = pl.ds(pl.multiple_of(j * width, lanes), width)
        valid = m_ref[:, cols] > 0
        out = []
        for b in range(bands):
            x = x_ref[b, :, cols].astype(jnp.float32)
            marked = jnp.where(valid, x, sentinel)
            for d in range(dates):
                wide[d * bands + b : d * bands + b + 1, :] = marked[d : d + 1, :]
            out.append(carry[b] + jnp.where(valid, x, 0.0))
        sent[j] = wide[...].astype(jnp.bfloat16)
        out.append(carry[bands] + jnp.where(valid, 1.0, 0.0))
        return tuple(out)

    zero = jnp.zeros((dates, width), jnp.float32)
    sums = lax.fori_loop(0, n, mark, tuple(zero for _ in range(bands + 1)))
    got[me] = sent[me]

    lane = lax.broadcasted_iota(jnp.int32, (dates, lanes), 1)
    date = lax.broadcasted_iota(jnp.int32, (dates, lanes), 0)
    lane_row = lax.broadcasted_iota(jnp.int32, (1, lanes), 1)
    row = jnp.zeros((dates, lanes), jnp.float32)
    for b in range(bands):
        row = row + jnp.where(lane == date * slot + b, jnp.sum(sums[b], axis=1, keepdims=True), 0.0)
    own = (lane >= date * slot) & (lane < (date + 1) * slot)
    count_row = jnp.where(own, jnp.sum(sums[bands], axis=1, keepdims=True), 0.0)
    part[0:1, :] = jnp.sum(row, axis=0, keepdims=True)
    part[1:2, :] = jnp.sum(count_row, axis=0, keepdims=True)
    years = jnp.zeros((1, lanes), jnp.float32)
    for d in range(dates):
        year = jnp.full((1, lanes), days_ref[d], jnp.int32).astype(jnp.float32) / 365.0
        years = jnp.where((lane_row >= d * slot) & (lane_row < (d + 1) * slot), year, years)
    mean_row[1:2, :] = years

    def part_copy(r):
        return pltpu.make_async_remote_copy(
            src_ref=part,
            dst_ref=parts.at[r],
            send_sem=part_send.at[r],
            recv_sem=part_recv.at[r],
            device_id={"pix": lax.rem(pix + r, pixes)},
            device_id_type=MESH,
        )

    def data_copy(r):
        return pltpu.make_async_remote_copy(
            src_ref=sent.at[ahead(r)],
            dst_ref=got.at[me],
            send_sem=data_send.at[r],
            recv_sem=data_recv.at[r],
            device_id={"date": ahead(r)},
            device_id_type=MESH,
        )

    def mean_copy(r):
        return pltpu.make_async_remote_copy(
            src_ref=mean_row,
            dst_ref=mean_rows.at[me],
            send_sem=mean_send.at[r],
            recv_sem=mean_recv.at[r],
            device_id={"date": ahead(r)},
            device_id_type=MESH,
        )

    def code_copy(p, r):
        return pltpu.make_async_remote_copy(
            src_ref=code[p].at[me],
            dst_ref=code[p].at[me],
            send_sem=code_send.at[p, r],
            recv_sem=code_recv.at[p, r],
            device_id={"date": ahead(r)},
            device_id_type=MESH,
        )

    pl.semaphore_wait(barrier, len(stack_line) + len(plane) + pixes - 1)
    for r in plane:
        pl.semaphore_signal(plane_sem, inc=1, device_id={"date": ahead(r)}, device_id_type=MESH)
    for r in range(1, pixes):
        part_copy(r).start()
    for r in stack_line + plane:
        data_copy(r).start()

    csum_row = part[0:1, :]
    cnt_row = part[1:2, :]
    for r in range(1, pixes):
        part_copy(r).wait_recv()
        csum_row = csum_row + parts[r, 0:1, :]
        cnt_row = cnt_row + parts[r, 1:2, :]
    mean_row[0:1, :] = csum_row / jnp.maximum(cnt_row, 1.0)
    mean_rows[me] = mean_row[...]
    pl.semaphore_wait(plane_sem, len(plane))
    for r in range(1, n):
        mean_copy(r).start()
    @pl.when(lax.rem(pix, 2) == 1)
    def _():
        pl.delay(4700)

    for r in rest:
        data_copy(r).start()

    @pl.loop(1, n)
    def _(r):
        mean_copy(r).wait_recv()

    for row_index, tile_ref in ((0, mean_tile), (1, year_tile)):
        for j in range(n):
            stack[j : j + 1, :] = mean_rows[j, row_index : row_index + 1, :]
        turned = jnp.transpose(stack[...])
        for j in range(n):
            for d in range(dates):
                column = turned[d * slot : d * slot + bands, j : j + 1]
                tile_ref[j * dates + d] = jnp.broadcast_to(column, (bands, lanes))

    def trend(r, carry):
        j = behind(r)
        fill, s_zero, s_one, s_two, s_y, s_ty = carry
        block = got[j].astype(jnp.float32)
        for d in range(dates):
            x = block[d * bands : (d + 1) * bands, :]
            year = jnp.concatenate([year_tile[j * dates + d]] * (width // lanes), axis=1)
            mean = jnp.concatenate([mean_tile[j * dates + d]] * (width // lanes), axis=1)
            valid = x < 50.0
            y = jnp.where(valid, x - mean, 0.0)
            m = jnp.where(valid, 1.0, 0.0)
            tm = year * m
            s_zero = s_zero + m
            s_one = s_one + tm
            s_two = s_two + year * tm
            s_y = s_y + y
            s_ty = s_ty + year * y
            flip[r * dates + d] = jnp.where(valid, x, fill)
            fill = jnp.where(valid, fill, -fill)
        return (fill, s_zero, s_one, s_two, s_y, s_ty)

    def arrived(r, carry):
        data_copy(r).wait_recv()
        return trend(r, carry)

    half = total // 2
    blank = jnp.zeros((bands, width), jnp.float32)
    sums = trend(0, (blank + sentinel, blank, blank, blank, blank, blank))
    sums = lax.fori_loop(1, n // 2, arrived, sums)

    @pl.loop(0, width // lanes)
    def _(k):
        cols = pl.ds(pl.multiple_of(k * lanes, lanes), lanes)
        for i, value in enumerate(sort_network([flip[i, :, cols] for i in range(half)])):
            flip[i, :, cols] = value

    sums = lax.fori_loop(n // 2, n, arrived, sums)
    fill, s_zero, s_one, s_two, s_y, s_ty = sums
    first = s_zero + ridge
    slopes[...] = (first * s_ty - s_one * s_y) / (first * (s_two + ridge) - s_one * s_one)
    odd[...] = jnp.where(fill < 0.0, 1.0, 0.0)

    def encode(base, values):
        top = jnp.maximum(jnp.max(jnp.abs(values), axis=0, keepdims=True), 1e-30)
        power = jnp.floor(jnp.log2(top))
        whole = jnp.round(values * jnp.exp2(14.0 - power))
        coded[base : base + bands, :] = jnp.clip(whole, -32767.0, 32767.0)
        coded[base + bands : base + bands + 1, :] = power

    def decode(p, j):
        for k in range(spans[p] // lanes):
            values = code[p][j, :, k * lanes : (k + 1) * lanes].astype(jnp.int32).astype(jnp.float32)
            there = pl.ds(pl.multiple_of(j * width + starts[p] + k * lanes, lanes), lanes)
            for o in range(2):
                scale = jnp.exp2(values[o * slot + bands : o * slot + bands + 1, :] - 14.0)
                out_ref[o, :, there] = values[o * slot : o * slot + bands, :] * scale

    for p, span in enumerate(spans):

        @pl.loop(0, span // lanes)
        def _(k):
            cols = pl.ds(pl.multiple_of(starts[p] + k * lanes, lanes), lanes)
            here = pl.ds(pl.multiple_of(k * lanes, lanes), lanes)
            low = [flip[i, :, cols] for i in range(half)]
            high = sort_network([flip[half + i, :, cols] for i in range(half)])
            lower = None
            upper = None
            for i in range(half):
                a, b = low[i], high[half - 1 - i]
                small, large = jnp.minimum(a, b), jnp.maximum(a, b)
                lower = small if lower is None else jnp.maximum(lower, small)
                upper = large if upper is None else jnp.minimum(upper, large)
            median = jnp.where(odd[:, cols] > 0.5, lower, 0.5 * (lower + upper))
            encode(0, median)
            encode(slot, slopes[:, cols])
            code[p][me, :, here] = coded[...].astype(jnp.int32).astype(jnp.int16)

        @pl.loop(1, n)
        def _(r):
            code_copy(p, r).start()

    for p in range(len(spans)):
        decode(p, me)

        @pl.loop(1, n)
        def _(r):
            code_copy(p, r).wait_recv()
            decode(p, behind(r))

    for r in range(1, pixes):
        part_copy(r).wait_send()

    @pl.loop(1, n)
    def _(r):
        mean_copy(r).wait_send()
        data_copy(r).wait_send()
        for p in range(len(spans)):
            code_copy(p, r).wait_send()


def local(n, pixes, reflect, cloud_free, days):
    dates, bands, tile = reflect.shape
    width = tile // n
    spans = [width]
    group = 1
    while group * group * 4 <= n and n % (group * 2) == 0:
        group *= 2
    turned = -(-n // lanes) * lanes
    vmem = pl.BlockSpec(memory_space=pltpu.VMEM)
    hbm = pl.BlockSpec(memory_space=pl.ANY)
    dma = pltpu.SemaphoreType.DMA
    out = pl.pallas_call(
        functools.partial(kernel, n, pixes, group, spans),
        out_shape=pltpu.VMEM((2, bands, tile), jnp.float32),
        in_specs=[hbm, hbm, pl.BlockSpec(memory_space=pltpu.SMEM)],
        out_specs=vmem,
        scratch_shapes=[
            pltpu.VMEM((bands, dates, tile), jnp.bfloat16),
            pltpu.VMEM((dates, tile), jnp.int32),
            pltpu.VMEM((dates * bands, width), jnp.float32),
            pltpu.VMEM((n, dates * bands, width), jnp.bfloat16),
            pltpu.VMEM((n, dates * bands, width), jnp.bfloat16),
            pltpu.VMEM((2, lanes), jnp.float32),
            pltpu.VMEM((pixes, 2, lanes), jnp.float32),
            pltpu.VMEM((2, lanes), jnp.float32),
            pltpu.VMEM((n, 2, lanes), jnp.float32),
            pltpu.VMEM((turned, lanes), jnp.float32),
            pltpu.VMEM((n * dates, bands, lanes), jnp.float32),
            pltpu.VMEM((n * dates, bands, lanes), jnp.float32),
            pltpu.VMEM((n * dates, bands, width), jnp.float32),
            pltpu.VMEM((bands, width), jnp.float32),
            pltpu.VMEM((bands, width), jnp.float32),
            pltpu.VMEM((2 * slot, lanes), jnp.float32),
            pltpu.SemaphoreType.REGULAR,
            dma((2,)),
            dma((n,)),
            dma((n,)),
            dma((pixes,)),
            dma((pixes,)),
            dma((n,)),
            dma((n,)),
            dma((len(spans), n)),
            dma((len(spans), n)),
            *[pltpu.VMEM((n, 2 * slot, span), jnp.int16) for span in spans],
        ],
        compiler_params=pltpu.CompilerParams(collective_id=0, has_side_effects=True),
    )(jnp.transpose(reflect, (1, 0, 2)), cloud_free, days)
    return (out[0], out[1])


def solution(mesh):
    placed = (P("date", None, "pix"), P("date", "pix"), P("date"))
    return jax.shard_map(
        functools.partial(local, mesh.shape["date"], mesh.shape["pix"]),
        mesh=mesh,
        in_specs=placed,
        out_specs=(P(None, "pix"), P(None, "pix")),
        check_vma=False,
    )
```

```python
import functools

import jax
import jax.numpy as jnp
from jax import lax
from jax.experimental import pallas as pl
from jax.experimental.pallas import tpu as pltpu
from jax.sharding import PartitionSpec as P

MESH = pl.DeviceIdType.MESH
ridge = 1.0
sentinel = 100.0
lanes = 128
slot = 8


def merge_pairs(lo, hi, r):
    step = r * 2
    if step < hi - lo:
        yield from merge_pairs(lo, hi, step)
        yield from merge_pairs(lo + r, hi, step)
        yield from ((i, i + r) for i in range(lo + r, hi - r, step))
    else:
        yield (lo, lo + r)


def sort_pairs(lo, hi):
    if hi - lo >= 1:
        mid = lo + (hi - lo) // 2
        yield from sort_pairs(lo, mid)
        yield from sort_pairs(mid + 1, hi)
        yield from merge_pairs(lo, hi, 1)


def sort_network(values):
    values = list(values)
    for i, j in sort_pairs(0, len(values) - 1):
        a, b = values[i], values[j]
        values[i], values[j] = jnp.minimum(a, b), jnp.maximum(a, b)
    return values


def kernel(
    n,
    pixes,
    group,
    spans,
    x_hbm,
    m_hbm,
    days_hbm,
    out_ref,
    x_ref,
    m_ref,
    wide,
    sent,
    got,
    part,
    parts,
    mean_row,
    mean_rows,
    stack,
    mean_tile,
    year_tile,
    flip,
    odd,
    slopes,
    coded,
    plane_sem,
    days_ref,
    load_sem,
    data_send,
    data_recv,
    part_send,
    part_recv,
    mean_send,
    mean_recv,
    code_send,
    code_recv,
    *code,
):
    me = lax.axis_index("date")
    pix = lax.axis_index("pix")
    bands, dates, tile = x_ref.shape
    width = tile // n
    total = n * dates
    starts = [sum(spans[:p]) for p in range(len(spans))]

    lines = n // group
    line = me // group
    spot = lax.rem(me, group)

    def ahead(r):
        return lax.rem(line + r // group, lines) * group + lax.rem(spot + lax.rem(r, group), group)

    def behind(r):
        return lax.rem(line + lines - r // group, lines) * group + lax.rem(spot + group - lax.rem(r, group), group)

    stack_line = [a * group for a in range(1, lines)]
    plane = list(range(1, group))
    rest = [r for r in range(1, n) if r not in stack_line and r not in plane]

    barrier = pltpu.get_barrier_semaphore()
    for r in stack_line + plane:
        pl.semaphore_signal(barrier, inc=1, device_id={"date": ahead(r)}, device_id_type=MESH)
    for r in range(1, pixes):
        pl.semaphore_signal(barrier, inc=1, device_id={"pix": lax.rem(pix + r, pixes)}, device_id_type=MESH)

    load_x = pltpu.make_async_copy(x_hbm, x_ref, load_sem.at[0])
    load_m = pltpu.make_async_copy(m_hbm, m_ref, load_sem.at[1])
    load_days = pltpu.make_async_copy(days_hbm, days_ref, load_sem.at[2])
    load_x.start()
    load_m.start()
    load_days.start()
    stack[...] = jnp.zeros_like(stack)
    coded[...] = jnp.zeros_like(coded)
    load_m.wait()
    load_x.wait()
    load_days.wait()

    def mark(j, carry):
        cols = pl.ds(pl.multiple_of(j * width, lanes), width)
        valid = m_ref[:, cols] > 0
        out = []
        for b in range(bands):
            x = x_ref[b, :, cols].astype(jnp.float32)
            marked = jnp.where(valid, x, sentinel)
            for d in range(dates):
                wide[d * bands + b : d * bands + b + 1, :] = marked[d : d + 1, :]
            out.append(carry[b] + jnp.where(valid, x, 0.0))
        sent[j] = wide[...].astype(jnp.bfloat16)
        out.append(carry[bands] + jnp.where(valid, 1.0, 0.0))
        return tuple(out)

    zero = jnp.zeros((dates, width), jnp.float32)
    sums = lax.fori_loop(0, n, mark, tuple(zero for _ in range(bands + 1)))
    got[me] = sent[me]

    lane = lax.broadcasted_iota(jnp.int32, (dates, lanes), 1)
    date = lax.broadcasted_iota(jnp.int32, (dates, lanes), 0)
    lane_row = lax.broadcasted_iota(jnp.int32, (1, lanes), 1)
    row = jnp.zeros((dates, lanes), jnp.float32)
    for b in range(bands):
        row = row + jnp.where(lane == date * slot + b, jnp.sum(sums[b], axis=1, keepdims=True), 0.0)
    own = (lane >= date * slot) & (lane < (date + 1) * slot)
    count_row = jnp.where(own, jnp.sum(sums[bands], axis=1, keepdims=True), 0.0)
    part[0:1, :] = jnp.sum(row, axis=0, keepdims=True)
    part[1:2, :] = jnp.sum(count_row, axis=0, keepdims=True)
    years = jnp.zeros((1, lanes), jnp.float32)
    for d in range(dates):
        year = jnp.full((1, lanes), days_ref[d], jnp.int32).astype(jnp.float32) / 365.0
        years = jnp.where((lane_row >= d * slot) & (lane_row < (d + 1) * slot), year, years)
    mean_row[1:2, :] = years

    def part_copy(r):
        return pltpu.make_async_remote_copy(
            src_ref=part,
            dst_ref=parts.at[r],
            send_sem=part_send.at[r],
            recv_sem=part_recv.at[r],
            device_id={"pix": lax.rem(pix + r, pixes)},
            device_id_type=MESH,
        )

    def data_copy(r):
        return pltpu.make_async_remote_copy(
            src_ref=sent.at[ahead(r)],
            dst_ref=got.at[me],
            send_sem=data_send.at[r],
            recv_sem=data_recv.at[r],
            device_id={"date": ahead(r)},
            device_id_type=MESH,
        )

    def mean_copy(r):
        return pltpu.make_async_remote_copy(
            src_ref=mean_row,
            dst_ref=mean_rows.at[me],
            send_sem=mean_send.at[r],
            recv_sem=mean_recv.at[r],
            device_id={"date": ahead(r)},
            device_id_type=MESH,
        )

    def code_copy(p, r):
        return pltpu.make_async_remote_copy(
            src_ref=code[p].at[me],
            dst_ref=code[p].at[me],
            send_sem=code_send.at[p, r],
            recv_sem=code_recv.at[p, r],
            device_id={"date": ahead(r)},
            device_id_type=MESH,
        )

    pl.semaphore_wait(barrier, len(stack_line) + len(plane) + pixes - 1)
    for r in plane:
        pl.semaphore_signal(plane_sem, inc=1, device_id={"date": ahead(r)}, device_id_type=MESH)
    for r in range(1, pixes):
        part_copy(r).start()
    for r in stack_line + plane:
        data_copy(r).start()

    csum_row = part[0:1, :]
    cnt_row = part[1:2, :]
    for r in range(1, pixes):
        part_copy(r).wait_recv()
        csum_row = csum_row + parts[r, 0:1, :]
        cnt_row = cnt_row + parts[r, 1:2, :]
    mean_row[0:1, :] = csum_row / jnp.maximum(cnt_row, 1.0)
    mean_rows[me] = mean_row[...]
    pl.semaphore_wait(plane_sem, len(plane))
    for r in range(1, n):
        mean_copy(r).start()
    @pl.when(lax.rem(pix, 2) == 1)
    def _():
        pl.delay(4700)

    for r in rest:
        data_copy(r).start()

    @pl.loop(1, n)
    def _(r):
        mean_copy(r).wait_recv()

    for row_index, tile_ref in ((0, mean_tile), (1, year_tile)):
        for j in range(n):
            stack[j : j + 1, :] = mean_rows[j, row_index : row_index + 1, :]
        turned = jnp.transpose(stack[...])
        for j in range(n):
            for d in range(dates):
                column = turned[d * slot : d * slot + bands, j : j + 1]
                tile_ref[j * dates + d] = jnp.broadcast_to(column, (bands, lanes))

    def trend(r, carry):
        j = behind(r)
        fill, s_zero, s_one, s_two, s_y, s_ty = carry
        block = got[j].astype(jnp.float32)
        for d in range(dates):
            x = block[d * bands : (d + 1) * bands, :]
            year = jnp.concatenate([year_tile[j * dates + d]] * (width // lanes), axis=1)
            mean = jnp.concatenate([mean_tile[j * dates + d]] * (width // lanes), axis=1)
            valid = x < 50.0
            y = jnp.where(valid, x - mean, 0.0)
            m = jnp.where(valid, 1.0, 0.0)
            tm = year * m
            s_zero = s_zero + m
            s_one = s_one + tm
            s_two = s_two + year * tm
            s_y = s_y + y
            s_ty = s_ty + year * y
            flip[r * dates + d] = jnp.where(valid, x, fill)
            fill = jnp.where(valid, fill, -fill)
        return (fill, s_zero, s_one, s_two, s_y, s_ty)

    def arrived(r, carry):
        data_copy(r).wait_recv()
        return trend(r, carry)

    half = total // 2
    blank = jnp.zeros((bands, width), jnp.float32)
    sums = trend(0, (blank + sentinel, blank, blank, blank, blank, blank))
    sums = lax.fori_loop(1, n // 2, arrived, sums)

    @pl.loop(0, width // lanes)
    def _(k):
        cols = pl.ds(pl.multiple_of(k * lanes, lanes), lanes)
        for i, value in enumerate(sort_network([flip[i, :, cols] for i in range(half)])):
            flip[i, :, cols] = value

    sums = lax.fori_loop(n // 2, n, arrived, sums)
    fill, s_zero, s_one, s_two, s_y, s_ty = sums
    first = s_zero + ridge
    slopes[...] = (first * s_ty - s_one * s_y) / (first * (s_two + ridge) - s_one * s_one)
    odd[...] = jnp.where(fill < 0.0, 1.0, 0.0)

    def encode(base, values):
        top = jnp.maximum(jnp.max(jnp.abs(values), axis=0, keepdims=True), 1e-30)
        power = jnp.floor(jnp.log2(top))
        whole = jnp.round(values * jnp.exp2(14.0 - power))
        coded[base : base + bands, :] = jnp.clip(whole, -32767.0, 32767.0)
        coded[base + bands : base + bands + 1, :] = power

    def decode(p, j):
        for k in range(spans[p] // lanes):
            values = code[p][j, :, k * lanes : (k + 1) * lanes].astype(jnp.int32).astype(jnp.float32)
            there = pl.ds(pl.multiple_of(j * width + starts[p] + k * lanes, lanes), lanes)
            for o in range(2):
                scale = jnp.exp2(values[o * slot + bands : o * slot + bands + 1, :] - 14.0)
                out_ref[o, :, there] = values[o * slot : o * slot + bands, :] * scale

    for p, span in enumerate(spans):

        @pl.loop(0, span // lanes)
        def _(k):
            cols = pl.ds(pl.multiple_of(starts[p] + k * lanes, lanes), lanes)
            here = pl.ds(pl.multiple_of(k * lanes, lanes), lanes)
            low = [flip[i, :, cols] for i in range(half)]
            high = sort_network([flip[half + i, :, cols] for i in range(half)])
            lower = None
            upper = None
            for i in range(half):
                a, b = low[i], high[half - 1 - i]
                small, large = jnp.minimum(a, b), jnp.maximum(a, b)
                lower = small if lower is None else jnp.maximum(lower, small)
                upper = large if upper is None else jnp.minimum(upper, large)
            median = jnp.where(odd[:, cols] > 0.5, lower, 0.5 * (lower + upper))
            encode(0, median)
            encode(slot, slopes[:, cols])
            code[p][me, :, here] = coded[...].astype(jnp.int32).astype(jnp.int16)

        for r in range(1, n):
            code_copy(p, r).start()

    for p in range(len(spans)):
        decode(p, me)

        for r in range(1, n, 3):
            some = range(r, min(r + 3, n))
            for q in some:
                code_copy(p, q).wait_recv()
            for q in some:
                decode(p, behind(q))

    for r in range(1, pixes):
        part_copy(r).wait_send()

    @pl.loop(1, n)
    def _(r):
        mean_copy(r).wait_send()
        data_copy(r).wait_send()
        for p in range(len(spans)):
            code_copy(p, r).wait_send()


def local(n, pixes, reflect, cloud_free, days):
    dates, bands, tile = reflect.shape
    width = tile // n
    spans = [width]
    group = 1
    while group * group * 4 <= n and n % (group * 2) == 0:
        group *= 2
    turned = -(-n // lanes) * lanes
    vmem = pl.BlockSpec(memory_space=pltpu.VMEM)
    hbm = pl.BlockSpec(memory_space=pl.ANY)
    dma = pltpu.SemaphoreType.DMA
    out = pl.pallas_call(
        functools.partial(kernel, n, pixes, group, spans),
        out_shape=pltpu.VMEM((2, bands, tile), jnp.float32),
        in_specs=[hbm, hbm, hbm],
        out_specs=vmem,
        scratch_shapes=[
            pltpu.VMEM((bands, dates, tile), jnp.bfloat16),
            pltpu.VMEM((dates, tile), jnp.int32),
            pltpu.VMEM((dates * bands, width), jnp.float32),
            pltpu.VMEM((n, dates * bands, width), jnp.bfloat16),
            pltpu.VMEM((n, dates * bands, width), jnp.bfloat16),
            pltpu.VMEM((2, lanes), jnp.float32),
            pltpu.VMEM((pixes, 2, lanes), jnp.float32),
            pltpu.VMEM((2, lanes), jnp.float32),
            pltpu.VMEM((n, 2, lanes), jnp.float32),
            pltpu.VMEM((turned, lanes), jnp.float32),
            pltpu.VMEM((n * dates, bands, lanes), jnp.float32),
            pltpu.VMEM((n * dates, bands, lanes), jnp.float32),
            pltpu.VMEM((n * dates, bands, width), jnp.float32),
            pltpu.VMEM((bands, width), jnp.float32),
            pltpu.VMEM((bands, width), jnp.float32),
            pltpu.VMEM((2 * slot, lanes), jnp.float32),
            pltpu.SemaphoreType.REGULAR,
            pltpu.SMEM((dates,), jnp.int32),
            dma((3,)),
            dma((n,)),
            dma((n,)),
            dma((pixes,)),
            dma((pixes,)),
            dma((n,)),
            dma((n,)),
            dma((len(spans), n)),
            dma((len(spans), n)),
            *[pltpu.VMEM((n, 2 * slot, span), jnp.int16) for span in spans],
        ],
        compiler_params=pltpu.CompilerParams(collective_id=0, has_side_effects=True),
    )(jnp.transpose(reflect, (1, 0, 2)), cloud_free, days)
    return (out[0], out[1])


def solution(mesh):
    placed = (P("date", None, "pix"), P("date", "pix"), P("date"))
    return jax.shard_map(
        functools.partial(local, mesh.shape["date"], mesh.shape["pix"]),
        mesh=mesh,
        in_specs=placed,
        out_specs=(P(None, "pix"), P(None, "pix")),
        check_vma=False,
    )
```

```python
import functools

import jax
import jax.numpy as jnp
from jax import lax
from jax.experimental import pallas as pl
from jax.experimental.pallas import tpu as pltpu
from jax.sharding import PartitionSpec as P

MESH = pl.DeviceIdType.MESH
ridge = 1.0
sentinel = 100.0
lanes = 128
slot = 8


def merge_pairs(lo, hi, r):
    step = r * 2
    if step < hi - lo:
        yield from merge_pairs(lo, hi, step)
        yield from merge_pairs(lo + r, hi, step)
        yield from ((i, i + r) for i in range(lo + r, hi - r, step))
    else:
        yield (lo, lo + r)


def sort_pairs(lo, hi):
    if hi - lo >= 1:
        mid = lo + (hi - lo) // 2
        yield from sort_pairs(lo, mid)
        yield from sort_pairs(mid + 1, hi)
        yield from merge_pairs(lo, hi, 1)


def sort_network(values):
    values = list(values)
    for i, j in sort_pairs(0, len(values) - 1):
        a, b = values[i], values[j]
        values[i], values[j] = jnp.minimum(a, b), jnp.maximum(a, b)
    return values


def kernel(
    n,
    pixes,
    group,
    spans,
    x_hbm,
    m_hbm,
    days_hbm,
    out_ref,
    x_ref,
    m_ref,
    wide,
    sent,
    got,
    part,
    parts,
    mean_row,
    mean_rows,
    stack,
    mean_tile,
    year_tile,
    flip,
    odd,
    slopes,
    coded,
    plane_sem,
    days_ref,
    load_sem,
    data_send,
    data_recv,
    part_send,
    part_recv,
    mean_send,
    mean_recv,
    code_send,
    code_recv,
    *code,
):
    me = lax.axis_index("date")
    pix = lax.axis_index("pix")
    bands, dates, tile = x_ref.shape
    width = tile // n
    total = n * dates
    starts = [sum(spans[:p]) for p in range(len(spans))]

    lines = n // group
    line = me // group
    spot = lax.rem(me, group)

    def ahead(r):
        return lax.rem(line + r // group, lines) * group + lax.rem(spot + lax.rem(r, group), group)

    def behind(r):
        return lax.rem(line + lines - r // group, lines) * group + lax.rem(spot + group - lax.rem(r, group), group)

    stack_line = [a * group for a in range(1, lines)]
    plane = list(range(1, group))
    rest = [r for r in range(1, n) if r not in stack_line and r not in plane]

    barrier = pltpu.get_barrier_semaphore()
    for r in stack_line + plane:
        pl.semaphore_signal(barrier, inc=1, device_id={"date": ahead(r)}, device_id_type=MESH)
    for r in range(1, pixes):
        pl.semaphore_signal(barrier, inc=1, device_id={"pix": lax.rem(pix + r, pixes)}, device_id_type=MESH)

    load_x = pltpu.make_async_copy(x_hbm, x_ref, load_sem.at[0])
    load_m = pltpu.make_async_copy(m_hbm, m_ref, load_sem.at[1])
    load_days = pltpu.make_async_copy(days_hbm, days_ref, load_sem.at[2])
    load_x.start()
    load_m.start()
    load_days.start()
    stack[...] = jnp.zeros_like(stack)
    coded[...] = jnp.zeros_like(coded)
    load_m.wait()
    load_x.wait()
    load_days.wait()

    def mark(j, carry):
        cols = pl.ds(pl.multiple_of(j * width, lanes), width)
        valid = m_ref[:, cols] > 0
        out = []
        for b in range(bands):
            x = x_ref[b, :, cols].astype(jnp.float32)
            marked = jnp.where(valid, x, sentinel)
            for d in range(dates):
                wide[d * bands + b : d * bands + b + 1, :] = marked[d : d + 1, :]
            out.append(carry[b] + jnp.where(valid, x, 0.0))
        sent[j] = wide[...].astype(jnp.bfloat16)
        out.append(carry[bands] + jnp.where(valid, 1.0, 0.0))
        return tuple(out)

    zero = jnp.zeros((dates, width), jnp.float32)
    sums = lax.fori_loop(0, n, mark, tuple(zero for _ in range(bands + 1)))
    got[me] = sent[me]

    lane = lax.broadcasted_iota(jnp.int32, (dates, lanes), 1)
    date = lax.broadcasted_iota(jnp.int32, (dates, lanes), 0)
    lane_row = lax.broadcasted_iota(jnp.int32, (1, lanes), 1)
    row = jnp.zeros((dates, lanes), jnp.float32)
    for b in range(bands):
        row = row + jnp.where(lane == date * slot + b, jnp.sum(sums[b], axis=1, keepdims=True), 0.0)
    own = (lane >= date * slot) & (lane < (date + 1) * slot)
    count_row = jnp.where(own, jnp.sum(sums[bands], axis=1, keepdims=True), 0.0)
    part[0:1, :] = jnp.sum(row, axis=0, keepdims=True)
    part[1:2, :] = jnp.sum(count_row, axis=0, keepdims=True)
    years = jnp.zeros((1, lanes), jnp.float32)
    for d in range(dates):
        year = jnp.full((1, lanes), days_ref[d], jnp.int32).astype(jnp.float32) / 365.0
        years = jnp.where((lane_row >= d * slot) & (lane_row < (d + 1) * slot), year, years)
    mean_row[1:2, :] = years

    def part_copy(r):
        return pltpu.make_async_remote_copy(
            src_ref=part,
            dst_ref=parts.at[r],
            send_sem=part_send.at[r],
            recv_sem=part_recv.at[r],
            device_id={"pix": lax.rem(pix + r, pixes)},
            device_id_type=MESH,
        )

    def data_copy(r):
        return pltpu.make_async_remote_copy(
            src_ref=sent.at[ahead(r)],
            dst_ref=got.at[me],
            send_sem=data_send.at[r],
            recv_sem=data_recv.at[r],
            device_id={"date": ahead(r)},
            device_id_type=MESH,
        )

    def mean_copy(r):
        return pltpu.make_async_remote_copy(
            src_ref=mean_row,
            dst_ref=mean_rows.at[me],
            send_sem=mean_send.at[r],
            recv_sem=mean_recv.at[r],
            device_id={"date": ahead(r)},
            device_id_type=MESH,
        )

    def code_copy(p, r):
        return pltpu.make_async_remote_copy(
            src_ref=code[p].at[me],
            dst_ref=code[p].at[me],
            send_sem=code_send.at[p, r],
            recv_sem=code_recv.at[p, r],
            device_id={"date": ahead(r)},
            device_id_type=MESH,
        )

    pl.semaphore_wait(barrier, len(stack_line) + len(plane) + pixes - 1)
    for r in plane:
        pl.semaphore_signal(plane_sem, inc=1, device_id={"date": ahead(r)}, device_id_type=MESH)
    for r in range(1, pixes):
        part_copy(r).start()
    for r in stack_line + plane:
        data_copy(r).start()

    def send_means():
        csum_row = part[0:1, :]
        cnt_row = part[1:2, :]
        for r in range(1, pixes):
            part_copy(r).wait_recv()
            csum_row = csum_row + parts[r, 0:1, :]
            cnt_row = cnt_row + parts[r, 1:2, :]
        mean_row[0:1, :] = csum_row / jnp.maximum(cnt_row, 1.0)
        mean_rows[me] = mean_row[...]
        for r in range(1, n):
            mean_copy(r).start()

    def send_rest():
        for r in rest:
            data_copy(r).start()

    pl.semaphore_wait(plane_sem, len(plane))

    @pl.when(lax.rem(pix, 2) == 0)
    def _():
        for r in rest[: len(rest) // 3]:
            data_copy(r).start()
        send_means()
        for r in rest[len(rest) // 3 :]:
            data_copy(r).start()

    @pl.when(lax.rem(pix, 2) == 1)
    def _():
        send_means()
        pl.delay(4700)
        send_rest()

    @pl.loop(1, n)
    def _(r):
        mean_copy(r).wait_recv()

    for row_index, tile_ref in ((0, mean_tile), (1, year_tile)):
        for j in range(n):
            stack[j : j + 1, :] = mean_rows[j, row_index : row_index + 1, :]
        turned = jnp.transpose(stack[...])
        for j in range(n):
            for d in range(dates):
                column = turned[d * slot : d * slot + bands, j : j + 1]
                tile_ref[j * dates + d] = jnp.broadcast_to(column, (bands, lanes))

    def trend(r, carry):
        j = behind(r)
        fill, s_zero, s_one, s_two, s_y, s_ty = carry
        block = got[j].astype(jnp.float32)
        for d in range(dates):
            x = block[d * bands : (d + 1) * bands, :]
            year = jnp.concatenate([year_tile[j * dates + d]] * (width // lanes), axis=1)
            mean = jnp.concatenate([mean_tile[j * dates + d]] * (width // lanes), axis=1)
            valid = x < 50.0
            y = jnp.where(valid, x - mean, 0.0)
            m = jnp.where(valid, 1.0, 0.0)
            tm = year * m
            s_zero = s_zero + m
            s_one = s_one + tm
            s_two = s_two + year * tm
            s_y = s_y + y
            s_ty = s_ty + year * y
            flip[r * dates + d] = jnp.where(valid, x, fill)
            fill = jnp.where(valid, fill, -fill)
        return (fill, s_zero, s_one, s_two, s_y, s_ty)

    def arrived(r, carry):
        data_copy(r).wait_recv()
        return trend(r, carry)

    half = total // 2
    blank = jnp.zeros((bands, width), jnp.float32)
    sums = trend(0, (blank + sentinel, blank, blank, blank, blank, blank))
    sums = lax.fori_loop(1, n // 2, arrived, sums)

    @pl.loop(0, width // lanes)
    def _(k):
        cols = pl.ds(pl.multiple_of(k * lanes, lanes), lanes)
        for i, value in enumerate(sort_network([flip[i, :, cols] for i in range(half)])):
            flip[i, :, cols] = value

    sums = lax.fori_loop(n // 2, n, arrived, sums)
    fill, s_zero, s_one, s_two, s_y, s_ty = sums
    first = s_zero + ridge
    slopes[...] = (first * s_ty - s_one * s_y) / (first * (s_two + ridge) - s_one * s_one)
    odd[...] = jnp.where(fill < 0.0, 1.0, 0.0)

    def encode(base, values):
        top = jnp.maximum(jnp.max(jnp.abs(values), axis=0, keepdims=True), 1e-30)
        power = jnp.floor(jnp.log2(top))
        whole = jnp.round(values * jnp.exp2(14.0 - power))
        coded[base : base + bands, :] = jnp.clip(whole, -32767.0, 32767.0)
        coded[base + bands : base + bands + 1, :] = power

    def decode(p, j):
        for k in range(spans[p] // lanes):
            values = code[p][j, :, k * lanes : (k + 1) * lanes].astype(jnp.int32).astype(jnp.float32)
            there = pl.ds(pl.multiple_of(j * width + starts[p] + k * lanes, lanes), lanes)
            for o in range(2):
                scale = jnp.exp2(values[o * slot + bands : o * slot + bands + 1, :] - 14.0)
                out_ref[o, :, there] = values[o * slot : o * slot + bands, :] * scale

    for p, span in enumerate(spans):

        @pl.loop(0, span // lanes)
        def _(k):
            cols = pl.ds(pl.multiple_of(starts[p] + k * lanes, lanes), lanes)
            here = pl.ds(pl.multiple_of(k * lanes, lanes), lanes)
            low = [flip[i, :, cols] for i in range(half)]
            high = sort_network([flip[half + i, :, cols] for i in range(half)])
            lower = None
            upper = None
            for i in range(half):
                a, b = low[i], high[half - 1 - i]
                small, large = jnp.minimum(a, b), jnp.maximum(a, b)
                lower = small if lower is None else jnp.maximum(lower, small)
                upper = large if upper is None else jnp.minimum(upper, large)
            median = jnp.where(odd[:, cols] > 0.5, lower, 0.5 * (lower + upper))
            odd[:, cols] = median

        encode(0, odd[...])
        encode(slot, slopes[...])
        code[p][me] = coded[...].astype(jnp.int32).astype(jnp.int16)
        for r in range(1, n):
            code_copy(p, r).start()

    for p in range(len(spans)):
        decode(p, me)

        for r in range(1, n, 3):
            some = range(r, min(r + 3, n))
            for q in some:
                code_copy(p, q).wait_recv()
            for q in some:
                decode(p, behind(q))

    for r in range(1, pixes):
        part_copy(r).wait_send()

    @pl.loop(1, n)
    def _(r):
        mean_copy(r).wait_send()
        data_copy(r).wait_send()
        for p in range(len(spans)):
            code_copy(p, r).wait_send()


def local(n, pixes, reflect, cloud_free, days):
    dates, bands, tile = reflect.shape
    width = tile // n
    spans = [width]
    group = 1
    while group * group * 4 <= n and n % (group * 2) == 0:
        group *= 2
    turned = -(-n // lanes) * lanes
    vmem = pl.BlockSpec(memory_space=pltpu.VMEM)
    hbm = pl.BlockSpec(memory_space=pl.ANY)
    dma = pltpu.SemaphoreType.DMA
    out = pl.pallas_call(
        functools.partial(kernel, n, pixes, group, spans),
        out_shape=pltpu.VMEM((2, bands, tile), jnp.float32),
        in_specs=[hbm, hbm, hbm],
        out_specs=vmem,
        scratch_shapes=[
            pltpu.VMEM((bands, dates, tile), jnp.bfloat16),
            pltpu.VMEM((dates, tile), jnp.int32),
            pltpu.VMEM((dates * bands, width), jnp.float32),
            pltpu.VMEM((n, dates * bands, width), jnp.bfloat16),
            pltpu.VMEM((n, dates * bands, width), jnp.bfloat16),
            pltpu.VMEM((2, lanes), jnp.float32),
            pltpu.VMEM((pixes, 2, lanes), jnp.float32),
            pltpu.VMEM((2, lanes), jnp.float32),
            pltpu.VMEM((n, 2, lanes), jnp.float32),
            pltpu.VMEM((turned, lanes), jnp.float32),
            pltpu.VMEM((n * dates, bands, lanes), jnp.float32),
            pltpu.VMEM((n * dates, bands, lanes), jnp.float32),
            pltpu.VMEM((n * dates, bands, width), jnp.float32),
            pltpu.VMEM((bands, width), jnp.float32),
            pltpu.VMEM((bands, width), jnp.float32),
            pltpu.VMEM((2 * slot, width), jnp.float32),
            pltpu.SemaphoreType.REGULAR,
            pltpu.SMEM((dates,), jnp.int32),
            dma((3,)),
            dma((n,)),
            dma((n,)),
            dma((pixes,)),
            dma((pixes,)),
            dma((n,)),
            dma((n,)),
            dma((len(spans), n)),
            dma((len(spans), n)),
            *[pltpu.VMEM((n, 2 * slot, span), jnp.int16) for span in spans],
        ],
        compiler_params=pltpu.CompilerParams(collective_id=0, has_side_effects=True),
    )(jnp.transpose(reflect, (1, 0, 2)), cloud_free, days)
    return (out[0], out[1])


def solution(mesh):
    placed = (P("date", None, "pix"), P("date", "pix"), P("date"))
    return jax.shard_map(
        functools.partial(local, mesh.shape["date"], mesh.shape["pix"]),
        mesh=mesh,
        in_specs=placed,
        out_specs=(P(None, "pix"), P(None, "pix")),
        check_vma=False,
    )
```

```python
import functools

import jax
import jax.numpy as jnp
from jax import lax
from jax.experimental import pallas as pl
from jax.experimental.pallas import tpu as pltpu
from jax.sharding import PartitionSpec as P

MESH = pl.DeviceIdType.MESH
ridge = 1.0
sentinel = 100.0
lanes = 128
slot = 8


def merge_pairs(lo, hi, r):
    step = r * 2
    if step < hi - lo:
        yield from merge_pairs(lo, hi, step)
        yield from merge_pairs(lo + r, hi, step)
        yield from ((i, i + r) for i in range(lo + r, hi - r, step))
    else:
        yield (lo, lo + r)


def sort_pairs(lo, hi):
    if hi - lo >= 1:
        mid = lo + (hi - lo) // 2
        yield from sort_pairs(lo, mid)
        yield from sort_pairs(mid + 1, hi)
        yield from merge_pairs(lo, hi, 1)


def sort_network(values):
    values = list(values)
    for i, j in sort_pairs(0, len(values) - 1):
        a, b = values[i], values[j]
        values[i], values[j] = jnp.minimum(a, b), jnp.maximum(a, b)
    return values


def kernel(
    n,
    pixes,
    group,
    spans,
    x_hbm,
    m_hbm,
    days_hbm,
    out_ref,
    x_ref,
    m_ref,
    wide,
    sent,
    got,
    part,
    parts,
    mean_row,
    mean_rows,
    stack,
    mean_tile,
    year_tile,
    flip,
    odd,
    slopes,
    coded,
    plane_sem,
    days_ref,
    load_sem,
    data_send,
    data_recv,
    part_send,
    part_recv,
    mean_send,
    mean_recv,
    code_send,
    code_recv,
    *code,
):
    me = lax.axis_index("date")
    pix = lax.axis_index("pix")
    bands, dates, tile = x_ref.shape
    width = tile // n
    total = n * dates
    starts = [sum(spans[:p]) for p in range(len(spans))]

    lines = n // group
    line = me // group
    spot = lax.rem(me, group)

    def ahead(r):
        return lax.rem(line + r // group, lines) * group + lax.rem(spot + lax.rem(r, group), group)

    def behind(r):
        return lax.rem(line + lines - r // group, lines) * group + lax.rem(spot + group - lax.rem(r, group), group)

    stack_line = [a * group for a in range(1, lines)]
    plane = list(range(1, group))
    rest = [r for r in range(1, n) if r not in stack_line and r not in plane]

    barrier = pltpu.get_barrier_semaphore()
    for r in stack_line + plane:
        pl.semaphore_signal(barrier, inc=1, device_id={"date": ahead(r)}, device_id_type=MESH)
    for r in range(1, pixes):
        pl.semaphore_signal(barrier, inc=1, device_id={"pix": lax.rem(pix + r, pixes)}, device_id_type=MESH)

    load_x = pltpu.make_async_copy(x_hbm, x_ref, load_sem.at[0])
    load_m = pltpu.make_async_copy(m_hbm, m_ref, load_sem.at[1])
    load_days = pltpu.make_async_copy(days_hbm, days_ref, load_sem.at[2])
    load_x.start()
    load_m.start()
    load_days.start()
    stack[...] = jnp.zeros_like(stack)
    coded[...] = jnp.zeros_like(coded)
    load_m.wait()
    load_x.wait()
    load_days.wait()

    def mark(j, carry):
        cols = pl.ds(pl.multiple_of(j * width, lanes), width)
        valid = m_ref[:, cols] > 0
        out = []
        for b in range(bands):
            x = x_ref[b, :, cols].astype(jnp.float32)
            marked = jnp.where(valid, x, sentinel)
            for d in range(dates):
                wide[d * bands + b : d * bands + b + 1, :] = marked[d : d + 1, :]
            out.append(carry[b] + jnp.where(valid, x, 0.0))
        sent[j] = wide[...].astype(jnp.bfloat16)
        out.append(carry[bands] + jnp.where(valid, 1.0, 0.0))
        return tuple(out)

    zero = jnp.zeros((dates, width), jnp.float32)
    sums = lax.fori_loop(0, n, mark, tuple(zero for _ in range(bands + 1)))
    got[me] = sent[me]

    lane = lax.broadcasted_iota(jnp.int32, (dates, lanes), 1)
    date = lax.broadcasted_iota(jnp.int32, (dates, lanes), 0)
    lane_row = lax.broadcasted_iota(jnp.int32, (1, lanes), 1)
    row = jnp.zeros((dates, lanes), jnp.float32)
    for b in range(bands):
        row = row + jnp.where(lane == date * slot + b, jnp.sum(sums[b], axis=1, keepdims=True), 0.0)
    own = (lane >= date * slot) & (lane < (date + 1) * slot)
    count_row = jnp.where(own, jnp.sum(sums[bands], axis=1, keepdims=True), 0.0)
    part[0:1, :] = jnp.sum(row, axis=0, keepdims=True)
    part[1:2, :] = jnp.sum(count_row, axis=0, keepdims=True)
    years = jnp.zeros((1, lanes), jnp.float32)
    for d in range(dates):
        year = jnp.full((1, lanes), days_ref[d], jnp.int32).astype(jnp.float32) / 365.0
        years = jnp.where((lane_row >= d * slot) & (lane_row < (d + 1) * slot), year, years)
    mean_row[1:2, :] = years

    def part_copy(r):
        return pltpu.make_async_remote_copy(
            src_ref=part,
            dst_ref=parts.at[r],
            send_sem=part_send.at[r],
            recv_sem=part_recv.at[r],
            device_id={"pix": lax.rem(pix + r, pixes)},
            device_id_type=MESH,
        )

    def data_copy(r):
        return pltpu.make_async_remote_copy(
            src_ref=sent.at[ahead(r)],
            dst_ref=got.at[me],
            send_sem=data_send.at[r],
            recv_sem=data_recv.at[r],
            device_id={"date": ahead(r)},
            device_id_type=MESH,
        )

    def mean_copy(r):
        return pltpu.make_async_remote_copy(
            src_ref=mean_row,
            dst_ref=mean_rows.at[me],
            send_sem=mean_send.at[r],
            recv_sem=mean_recv.at[r],
            device_id={"date": ahead(r)},
            device_id_type=MESH,
        )

    def code_copy(p, r):
        return pltpu.make_async_remote_copy(
            src_ref=code[p].at[me],
            dst_ref=code[p].at[me],
            send_sem=code_send.at[p, r],
            recv_sem=code_recv.at[p, r],
            device_id={"date": ahead(r)},
            device_id_type=MESH,
        )

    pl.semaphore_wait(barrier, len(stack_line) + len(plane) + pixes - 1)
    for r in plane:
        pl.semaphore_signal(plane_sem, inc=1, device_id={"date": ahead(r)}, device_id_type=MESH)
    for r in range(1, pixes):
        part_copy(r).start()
    for r in stack_line + plane:
        data_copy(r).start()

    def send_means():
        csum_row = part[0:1, :]
        cnt_row = part[1:2, :]
        for r in range(1, pixes):
            part_copy(r).wait_recv()
            csum_row = csum_row + parts[r, 0:1, :]
            cnt_row = cnt_row + parts[r, 1:2, :]
        mean_row[0:1, :] = csum_row / jnp.maximum(cnt_row, 1.0)
        mean_rows[me] = mean_row[...]
        for r in range(1, n):
            mean_copy(r).start()

    def send_rest():
        for r in rest:
            data_copy(r).start()

    pl.semaphore_wait(plane_sem, len(plane))

    @pl.when(lax.rem(pix, 2) == 0)
    def _():
        for r in rest[: len(rest) // 3]:
            data_copy(r).start()
        send_means()
        for r in rest[len(rest) // 3 :]:
            data_copy(r).start()

    @pl.when(lax.rem(pix, 2) == 1)
    def _():
        send_means()
        pl.delay(4700)
        send_rest()

    @pl.loop(1, n)
    def _(r):
        mean_copy(r).wait_recv()

    for row_index, tile_ref in ((0, mean_tile), (1, year_tile)):
        for j in range(n):
            stack[j : j + 1, :] = mean_rows[j, row_index : row_index + 1, :]
        turned = jnp.transpose(stack[...])
        for j in range(n):
            for d in range(dates):
                column = turned[d * slot : d * slot + bands, j : j + 1]
                tile_ref[j * dates + d] = jnp.broadcast_to(column, (bands, lanes))

    def trend(r, carry):
        j = behind(r)
        fill, s_zero, s_one, s_two, s_y, s_ty = carry
        block = got[j].astype(jnp.float32)
        for d in range(dates):
            x = block[d * bands : (d + 1) * bands, :]
            year = jnp.concatenate([year_tile[j * dates + d]] * (width // lanes), axis=1)
            mean = jnp.concatenate([mean_tile[j * dates + d]] * (width // lanes), axis=1)
            valid = x < 50.0
            y = jnp.where(valid, x - mean, 0.0)
            m = jnp.where(valid, 1.0, 0.0)
            tm = year * m
            s_zero = s_zero + m
            s_one = s_one + tm
            s_two = s_two + year * tm
            s_y = s_y + y
            s_ty = s_ty + year * y
            flip[r * dates + d] = jnp.where(valid, x, fill)
            fill = jnp.where(valid, fill, -fill)
        return (fill, s_zero, s_one, s_two, s_y, s_ty)

    def arrived(r, carry):
        data_copy(r).wait_recv()
        return trend(r, carry)

    half = total // 2
    blank = jnp.zeros((bands, width), jnp.float32)
    sums = trend(0, (blank + sentinel, blank, blank, blank, blank, blank))
    sums = lax.fori_loop(1, n // 2, arrived, sums)

    @pl.loop(0, width // lanes)
    def _(k):
        cols = pl.ds(pl.multiple_of(k * lanes, lanes), lanes)
        for i, value in enumerate(sort_network([flip[i, :, cols] for i in range(half)])):
            flip[i, :, cols] = value

    sums = lax.fori_loop(n // 2, n, arrived, sums)
    fill, s_zero, s_one, s_two, s_y, s_ty = sums
    first = s_zero + ridge
    slopes[...] = (first * s_ty - s_one * s_y) / (first * (s_two + ridge) - s_one * s_one)
    odd[...] = jnp.where(fill < 0.0, 1.0, 0.0)

    def encode(base, values):
        top = jnp.maximum(jnp.max(jnp.abs(values), axis=0, keepdims=True), 1e-30)
        power = jnp.floor(jnp.log2(top))
        whole = jnp.round(values * jnp.exp2(14.0 - power))
        coded[base : base + bands, :] = jnp.clip(whole, -32767.0, 32767.0)
        coded[base + bands : base + bands + 1, :] = power

    def decode(p, j):
        for k in range(spans[p] // lanes):
            values = code[p][j, :, k * lanes : (k + 1) * lanes].astype(jnp.int32).astype(jnp.float32)
            there = pl.ds(pl.multiple_of(j * width + starts[p] + k * lanes, lanes), lanes)
            for o in range(2):
                scale = jnp.exp2(values[o * slot + bands : o * slot + bands + 1, :] - 14.0)
                out_ref[o, :, there] = values[o * slot : o * slot + bands, :] * scale

    for p, span in enumerate(spans):

        @pl.loop(0, span // lanes)
        def _(k):
            cols = pl.ds(pl.multiple_of(starts[p] + k * lanes, lanes), lanes)
            here = pl.ds(pl.multiple_of(k * lanes, lanes), lanes)
            low = [flip[i, :, cols] for i in range(half)]
            high = sort_network([flip[half + i, :, cols] for i in range(half)])
            lower = None
            upper = None
            for i in range(half):
                a, b = low[i], high[half - 1 - i]
                small, large = jnp.minimum(a, b), jnp.maximum(a, b)
                lower = small if lower is None else jnp.maximum(lower, small)
                upper = large if upper is None else jnp.minimum(upper, large)
            median = jnp.where(odd[:, cols] > 0.5, lower, 0.5 * (lower + upper))
            odd[:, cols] = median

        encode(0, odd[...])
        encode(slot, slopes[...])
        code[p][me] = coded[...].astype(jnp.int32).astype(jnp.int16)
        for r in range(1, n):
            code_copy(p, r).start()

    for p in range(len(spans)):
        decode(p, me)

        for r in range(1, n, 5):
            some = range(r, min(r + 5, n))
            for q in some:
                code_copy(p, q).wait_recv()
            for q in some:
                decode(p, behind(q))

    for r in range(1, pixes):
        part_copy(r).wait_send()

    @pl.loop(1, n)
    def _(r):
        mean_copy(r).wait_send()
        data_copy(r).wait_send()
        for p in range(len(spans)):
            code_copy(p, r).wait_send()


def local(n, pixes, reflect, cloud_free, days):
    dates, bands, tile = reflect.shape
    width = tile // n
    spans = [width]
    group = 1
    while group * group * 4 <= n and n % (group * 2) == 0:
        group *= 2
    turned = -(-n // lanes) * lanes
    vmem = pl.BlockSpec(memory_space=pltpu.VMEM)
    hbm = pl.BlockSpec(memory_space=pl.ANY)
    dma = pltpu.SemaphoreType.DMA
    out = pl.pallas_call(
        functools.partial(kernel, n, pixes, group, spans),
        out_shape=pltpu.VMEM((2, bands, tile), jnp.float32),
        in_specs=[hbm, hbm, hbm],
        out_specs=vmem,
        scratch_shapes=[
            pltpu.VMEM((bands, dates, tile), jnp.bfloat16),
            pltpu.VMEM((dates, tile), jnp.int32),
            pltpu.VMEM((dates * bands, width), jnp.float32),
            pltpu.VMEM((n, dates * bands, width), jnp.bfloat16),
            pltpu.VMEM((n, dates * bands, width), jnp.bfloat16),
            pltpu.VMEM((2, lanes), jnp.float32),
            pltpu.VMEM((pixes, 2, lanes), jnp.float32),
            pltpu.VMEM((2, lanes), jnp.float32),
            pltpu.VMEM((n, 2, lanes), jnp.float32),
            pltpu.VMEM((turned, lanes), jnp.float32),
            pltpu.VMEM((n * dates, bands, lanes), jnp.float32),
            pltpu.VMEM((n * dates, bands, lanes), jnp.float32),
            pltpu.VMEM((n * dates, bands, width), jnp.float32),
            pltpu.VMEM((bands, width), jnp.float32),
            pltpu.VMEM((bands, width), jnp.float32),
            pltpu.VMEM((2 * slot, width), jnp.float32),
            pltpu.SemaphoreType.REGULAR,
            pltpu.SMEM((dates,), jnp.int32),
            dma((3,)),
            dma((n,)),
            dma((n,)),
            dma((pixes,)),
            dma((pixes,)),
            dma((n,)),
            dma((n,)),
            dma((len(spans), n)),
            dma((len(spans), n)),
            *[pltpu.VMEM((n, 2 * slot, span), jnp.int16) for span in spans],
        ],
        compiler_params=pltpu.CompilerParams(collective_id=0, has_side_effects=True),
    )(jnp.transpose(reflect, (1, 0, 2)), cloud_free, days)
    return (out[0], out[1])


def solution(mesh):
    placed = (P("date", None, "pix"), P("date", "pix"), P("date"))
    return jax.shard_map(
        functools.partial(local, mesh.shape["date"], mesh.shape["pix"]),
        mesh=mesh,
        in_specs=placed,
        out_specs=(P(None, "pix"), P(None, "pix")),
        check_vma=False,
    )
```
